128 devices in a mesh: rep: 1, dp: 128 (over x, y, z, core).
Axes of the slice: x: 4, y: 4, z: 4, core: 2. Of those that a mesh axis runs over, the one named last changes fastest.
Arguments:
- g_w_gate: bfloat16 [128, 2, 640, 2048], P(('rep', 'dp'))
- g_w_up: bfloat16 [128, 2, 640, 2048], P(('rep', 'dp'))
- g_w_down: bfloat16 [128, 2, 2048, 640], P(('rep', 'dp'))
- w_gate: bfloat16 [2, 640, 2048], replicated
- w_up: bfloat16 [2, 640, 2048], replicated
- w_down: bfloat16 [2, 2048, 640], replicated
- m_w_gate: float32 [2, 640, 2048], P(None, 'dp')
- m_w_up: float32 [2, 640, 2048], P(None, 'dp')
- m_w_down: float32 [2, 2048, 640], P(None, 'dp')
- v_w_gate: float32 [2, 640, 2048], P(None, 'dp')
- v_w_up: float32 [2, 640, 2048], P(None, 'dp')
- v_w_down: float32 [2, 2048, 640], P(None, 'dp')
Outputs:
- output 1: bfloat16 [2, 640, 2048], P('rep')
- output 2: bfloat16 [2, 640, 2048], P('rep')
- output 3: bfloat16 [2, 2048, 640], P('rep')
- output 4: float32 [2, 640, 2048], P('rep', 'dp')
- output 5: float32 [2, 640, 2048], P('rep', 'dp')
- output 6: float32 [2, 2048, 640], P('rep', 'dp')
- output 7: float32 [2, 640, 2048], P('rep', 'dp')
- output 8: float32 [2, 640, 2048], P('rep', 'dp')
- output 9: float32 [2, 2048, 640], P('rep', 'dp')
All inputs are finite; a program needn't handle non-finite values.
Results may differ from the reference program's by a relative error of at most 0.022.
Values are sent between devices in bfloat16 or wider.
A program may use at most 1.5 GiB of HBM per device.

```python
import jax
import jax.numpy as jnp
from jax import lax

DEVICES = 128
D = 640
FF = 2048
LAYERS = 2
NAMES = ("w_gate", "w_up", "w_down")
SHAPES = {"w_gate": (LAYERS, D, FF), "w_up": (LAYERS, D, FF), "w_down": (LAYERS, FF, D)}


def setup_inputs(seed: int = 0, part: int = 0) -> dict:
    kz, *keys = jax.random.split(jax.random.key(seed), 1 + 5 * len(NAMES))
    loud = 2.0 ** jax.random.uniform(kz, (), jnp.float32, -1.0, 1.0)
    drawn = {}
    for name, key, both in zip(NAMES, keys[:3], keys[3:6], strict=True):
        own = jax.random.normal(jax.random.fold_in(key, part), (DEVICES, *SHAPES[name]), jnp.float32)
        shared = jax.random.normal(jax.random.fold_in(both, part), SHAPES[name], jnp.float32)
        drawn["g_" + name] = (loud * (0.7 * shared / DEVICES + 0.7 * own * DEVICES**-0.5)).astype(jnp.bfloat16)
    for name, key in zip(NAMES, keys[6:9], strict=True):
        drawn[name] = (jax.random.normal(key, SHAPES[name], jnp.float32) * SHAPES[name][1] ** -0.5).astype(jnp.bfloat16)
    for name, key in zip(NAMES, keys[9:12], strict=True):
        drawn["m_" + name] = loud * 0.5 * jax.random.normal(key, SHAPES[name], jnp.float32)
    for name, key in zip(NAMES, keys[12:15], strict=True):
        drawn["v_" + name] = loud * loud * jax.random.uniform(key, SHAPES[name], jnp.float32, 0.5, 1.5)
    return drawn


def adamw(w, m, v, g):
    m = 0.9 * m + 0.1 * g
    v = 0.95 * v + 0.05 * g * g
    step = m * lax.rsqrt(v + 1e-8) + 0.1 * w
    return (w - 0.02 * step).astype(jnp.bfloat16), m, v


def reference(g_w_gate, g_w_up, g_w_down, w_gate, w_up, w_down, m_w_gate, m_w_up, m_w_down, v_w_gate, v_w_up, v_w_down):
    def total(terms):
        return lax.scan(lambda so_far, term: (so_far + term.astype(jnp.float32), None), jnp.zeros(terms.shape[1:], jnp.float32), terms)[0]

    gradients = [total(terms).astype(jnp.bfloat16).astype(jnp.float32) for terms in (g_w_gate, g_w_up, g_w_down)]
    new = [
        adamw(w.astype(jnp.float32), m, v, g)
        for w, m, v, g in zip((w_gate, w_up, w_down), (m_w_gate, m_w_up, m_w_down), (v_w_gate, v_w_up, v_w_down), gradients, strict=True)
    ]
    return tuple(one[which] for which in range(3) for one in new)
```

```python
import jax
import jax.numpy as jnp
from jax import lax
from jax.experimental import pallas as pl
from jax.experimental.pallas import tpu as pltpu
from jax.sharding import PartitionSpec as P

F32, BF16 = jnp.float32, jnp.bfloat16
MESH = pl.DeviceIdType.MESH
COPIES = 224
WIDE, TALL = (2, 4, 4, 5, 2, 64, 128), (2, 4, 4, 4, 2, 80, 128)
HALF = ((2, 4, 4, 5, 64, 128), (2, 4, 4, 5, 64, 128), (2, 4, 4, 4, 80, 128))
SHARD = (
    ((4, 5, 64, 128), (5, 64, 128), (5, 16, 128)),
    ((4, 5, 64, 128), (4, 5, 16, 128), (5, 16, 128)),
    ((4, 4, 80, 128), (4, 80, 128), (80, 128)),
)
AXES = (("x", "y", "z"), ("y", "z", "x"), ("z", "x", "y"))
SMALL = ((5, 32, 128), (5, 32, 128), (2, 80, 128))


def adamw(w, m, v, g):
    m = 0.9 * m + 0.1 * g
    v = 0.95 * v + 0.05 * g * g
    step = m * lax.rsqrt(v + 1e-8) + 0.1 * w
    return w - 0.02 * step, m, v


def add_into(dst, *others):
    def at(index):
        total = dst[index].astype(F32)
        for one in others:
            total = total + one[index].astype(F32)
        dst[index] = total.astype(BF16)

    lead = dst.shape[:-2]
    if len(lead) < 2:
        for i in range(lead[0] if lead else 1):
            at((i,) if lead else ())
        return

    @pl.loop(0, lead[0])
    def _(i):
        for j in range(lead[1]):
            at((i, j))


def kernel(*refs):
    grads, weights, ms, vs = (refs[i : i + 3] for i in (0, 3, 6, 9))
    outs, new_ms, new_vs = (refs[i : i + 3] for i in (12, 15, 18))
    own, other, gathered = (refs[i : i + 3] for i in (21, 24, 27))
    landing = (refs[30:33], refs[33:36], refs[36:39])
    m_in, v_in = refs[39:42], refs[42:45]
    rows, w_block, w_down, turned, out_box, in_box, back_out, back_in, send_sems, recv_sems, local_sems = refs[45:]

    me = lax.axis_index("dp")
    core = lax.rem(me, 2)
    pos = {"z": lax.rem(me // 2, 4), "y": lax.rem(me // 8, 4), "x": me // 32}
    d = 2 * pos["z"] + core

    def device(core=core, **moved):
        at = {**pos, **moved}
        return ((at["x"] * 4 + at["y"]) * 4 + at["z"]) * 2 + core

    def step(axis, by):
        return lax.rem(pos[axis] + by + 4, 4)

    partner = device(core=1 - core)
    right = {a: device(**{a: step(a, 1)}) for a in "xyz"}
    left = {a: device(**{a: step(a, -1)}) for a in "xyz"}
    line = [lax.rem(d + k, 8) for k in range(1, 8)]
    line_device = [device(core=lax.rem(t, 2), z=t // 2) for t in line]

    used = [0, 0]
    sent = []

    def send(src, dst, to):
        copy = pltpu.make_async_remote_copy(
            src_ref=src,
            dst_ref=dst,
            send_sem=send_sems.at[used[0]],
            recv_sem=recv_sems.at[used[0]],
            device_id={"dp": to},
            device_id_type=MESH,
        )
        used[0] += 1
        copy.start()
        sent.append(copy)
        return copy

    def local(src, dst):
        copy = pltpu.make_async_copy(src, dst, local_sems.at[used[1]])
        used[1] += 1
        copy.start()
        return copy

    def of_whole(ref, weight, layer, s, side):
        if weight == 0:
            return ref.at[layer, s, :, :, side]
        if weight == 1:
            return ref.at[layer, :, s, :, side]
        return ref.at[layer, :, :, s, side]

    def part(ref, weight, phase, layer, s):
        if phase == 0:
            return ref.at[layer, s]
        first = pos[AXES[weight][0]]
        if weight == 0:
            z = pl.ds(pl.multiple_of(16 * s, 16), 16)
            return ref.at[layer, first, s] if phase == 1 else ref.at[layer, first, pos["y"], :, z]
        if weight == 1:
            z = pl.ds(pl.multiple_of(16 * (s if phase == 1 else pos["z"]), 16), 16)
            return ref.at[layer, first, :, :, z] if phase == 1 else ref.at[layer, first, s, :, z]
        return ref.at[layer, first, s] if phase == 1 else ref.at[layer, first, pos["x"], s]

    order = (((2, 0), (2, 1)), ((1, 1), (-1, 0)), ((1, 0), (-1, 1)), ((0, 0), (0, 1)))
    loads = {}
    for group in order:
        for by, layer in group:
            for weight in range(3):
                s = step(AXES[weight][0], by)
                loads[weight, by, layer] = local(of_whole(grads[weight], weight, layer, s, core), own[weight].at[layer, s])
    x, y, z = pos["x"], pos["y"], pos["z"]
    small = [local(ms[i], m_in[i]) for i in range(3)] + [local(vs[i], v_in[i]) for i in range(3)]
    small += [local(weights[i].at[:, x, y], w_block.at[i]) for i in range(2)]
    small += [local(weights[2].at[:, x, y, z, core], w_down)]

    barrier = pltpu.get_barrier_semaphore()
    peers = [right["x"], left["x"], right["y"], left["y"], *line_device]
    for peer in peers:
        pl.semaphore_signal(barrier, inc=1, device_id={"dp": peer}, device_id_type=MESH)
    pl.semaphore_wait(barrier, len(peers))

    pairs = {}
    for group in order:
        for by, layer in group:
            for weight in range(3):
                s = step(AXES[weight][0], by)
                pairs[weight, by, layer] = send(
                    of_whole(grads[weight], weight, layer, s, 1 - core), other[weight].at[layer, s], partner
                )

    def pair_sum(weight, by, layer, *more):
        loads[weight, by, layer].wait()
        pairs[weight, by, layer].wait_recv()
        s = step(AXES[weight][0], by)
        add_into(own[weight].at[layer, s], other[weight].at[layer, s], *more)

    for phase in range(3):
        first, raw, summed = {}, {}, {}

        def shard(weight, by, layer, phase=phase):
            return part(own[weight], weight, phase, layer, step(AXES[weight][phase], by))

        def land(weight, which, layer, phase=phase):
            return landing[phase][weight].at[which, layer]

        def ways(weight, phase=phase):
            axis = AXES[weight][phase]
            return right[axis], left[axis]

        for weight in range(3):
            for layer in range(2):
                if phase == 0:
                    pair_sum(weight, 2, layer)
                first[weight, layer] = send(shard(weight, 2, layer), land(weight, 0, layer), ways(weight)[layer])
        for weight in range(3):
            for layer, by in ((1, 1), (0, -1)):
                if phase == 0:
                    pair_sum(weight, by, layer)
                raw[weight, layer] = send(shard(weight, by, layer), land(weight, 1, layer), ways(weight)[1 - layer])
        if phase == 0:
            for weight in range(3):
                for layer, by in ((0, 1), (1, -1)):
                    pair_sum(weight, by, layer)
        for weight in range(3):
            for layer, by in ((0, 1), (1, -1)):
                first[weight, layer].wait_recv()
                add_into(shard(weight, by, layer), land(weight, 0, layer))
                summed[weight, layer] = send(shard(weight, by, layer), land(weight, 2, layer), ways(weight)[layer])
        if phase == 0:
            for weight in range(3):
                for layer in range(2):
                    pair_sum(weight, 0, layer)
        if phase == 1:
            for one in small:
                one.wait()
            for weight in range(2):
                for layer in range(2):

                    @pl.loop(0, 5)
                    def _(i, weight=weight, layer=layer):
                        for side in range(2):
                            block = w_block[weight, layer, i, side].astype(F32)
                            for t in range(8):
                                start = 256 * i + 2 * (8 * side + t) + layer
                                turned[weight, pl.ds(start, 8, 32), :] = block[8 * t : 8 * t + 8]
        for weight in range(3):
            for layer in range(2):
                raw[weight, layer].wait_recv()
                summed[weight, layer].wait_recv()
                add_into(shard(weight, 0, layer), land(weight, 1, layer), land(weight, 2, layer))

    for weight in range(2):
        for layer in range(2):
            block = part(own[weight], weight, 2, layer, pos[AXES[weight][2]])
            for i in range(5):
                both = block[i].astype(F32)
                for t in range(2):
                    rows[pl.ds(64 * i + 4 * weight + 2 * t + layer, 8, 8), :] = both[8 * t : 8 * t + 8]
    for t in range(8):
        out_box[t] = rows[40 * t : 40 * t + 40].reshape(5, 8, 128).astype(BF16)
    moves = [send(out_box.at[t], in_box.at[d], to) for t, to in zip(line, line_device)]
    in_box[d] = out_box[d]

    for layer in range(2):
        g = part(own[2], 2, 2, layer, pos["y"])[...].astype(F32)
        w, m, v = adamw(w_down[layer].astype(F32), m_in[2][layer], v_in[2][layer], g)
        m_in[2][layer] = m
        v_in[2][layer] = v
        gathered[2][layer, pos["z"], pos["x"], pos["y"]] = w.astype(BF16)

    for one in moves:
        one.wait_recv()
    low = lax.broadcasted_iota(jnp.int32, (8, 128), 0) < 4

    def swap(a, b):
        return jnp.where(low, a, pltpu.roll(b, 4, 0)), jnp.where(low, pltpu.roll(a, 4, 0), b)

    for side in range(2):
        for half in range(2):
            even, odd = 4 * half + side, 4 * half + 2 + side

            @pl.loop(0, 5)
            def _(r, side=side, half=half, even=even, odd=odd):
                new = []
                at = 8 * (2 * side + half)
                gs = swap(in_box[even, r].astype(F32), in_box[odd, r].astype(F32))
                for weight in range(2):
                    here = (r, pl.ds(at, 8))
                    w = turned[weight, pl.ds(pl.multiple_of(160 * d + 32 * r + at, 8), 8), :]
                    w, m, v = adamw(w, m_in[weight][here], v_in[weight][here], gs[weight])
                    m_in[weight][here] = m
                    v_in[weight][here] = v
                    new.append(w)
                to_even, to_odd = swap(*new)
                back_out[even, r] = to_even.astype(BF16)
                back_out[odd, r] = to_odd.astype(BF16)

    moves = [send(back_out.at[t], back_in.at[d], to) for t, to in zip(line, line_device)]
    back_in[d] = back_out[d]
    results = [local(m_in[i], new_ms[i]) for i in range(3)] + [local(v_in[i], new_vs[i]) for i in range(3)]
    for one in moves:
        one.wait_recv()
    for t in range(8):
        rows[40 * t : 40 * t + 40] = back_in[t].astype(F32).reshape(40, 128)
    for weight in range(2):
        for layer in range(2):
            block = part(gathered[weight], weight, 2, layer, pos[AXES[weight][2]])
            for i in range(5):
                both = [rows[pl.ds(64 * i + 4 * weight + 2 * t + layer, 8, 8), :] for t in range(2)]
                block[i] = jnp.concatenate(both, 0).astype(BF16)

    arrivals = []
    for phase in (2, 1, 0):
        firsts, lasts, forwards = {}, {}, {}

        def shard(weight, by, layer, phase=phase):
            return part(gathered[weight], weight, phase, layer, step(AXES[weight][phase], by))

        def spread(weight, by, layer, phase=phase):
            if phase == 0:
                s = step(AXES[weight][0], by)
                src = gathered[weight].at[layer, s]
                dst = of_whole(outs[weight], weight, layer, s, core)
                arrivals.append(send(src, dst, partner))
                results.append(local(src, dst))

        for weight in range(3):
            axis = AXES[weight][phase]
            for layer in range(2):
                firsts[weight, layer] = send(shard(weight, 0, layer), shard(weight, 0, layer), (right[axis], left[axis])[layer])
        for weight in range(3):
            axis = AXES[weight][phase]
            for layer in range(2):
                lasts[weight, layer] = send(shard(weight, 0, layer), shard(weight, 0, layer), (left[axis], right[axis])[layer])
        for weight in range(3):
            for layer in range(2):
                spread(weight, 0, layer)
        for weight in range(3):
            axis = AXES[weight][phase]
            for layer, by in ((0, -1), (1, 1)):
                firsts[weight, layer].wait_recv()
                forwards[weight, layer] = send(shard(weight, by, layer), shard(weight, by, layer), (right[axis], left[axis])[layer])
                spread(weight, by, layer)
        for weight in range(3):
            for layer, by in ((0, 1), (1, -1)):
                lasts[weight, layer].wait_recv()
                spread(weight, by, layer)
        for weight in range(3):
            for layer in range(2):
                forwards[weight, layer].wait_recv()
                spread(weight, 2, layer)

    for one in results:
        one.wait()
    for one in arrivals:
        one.wait_recv()
    for one in sent:
        one.wait_send()


def wide(a):
    return a.reshape(2, 80, 8, 16, 128).transpose(0, 1, 3, 2, 4).reshape(WIDE)


def tall(a):
    return a.reshape(2, 256, 8, 5, 128).transpose(0, 1, 3, 2, 4).reshape(TALL)


def wide_small(a):
    return a.transpose(1, 0, 2).reshape(5, 2, 16, 128).transpose(0, 2, 1, 3).reshape(5, 32, 128)


def tall_small(a):
    return a.reshape(2, 2, 8, 5, 128).transpose(0, 1, 3, 2, 4).reshape(2, 80, 128)


def unwide(a):
    return a.reshape(2, 80, 16, 8, 128).transpose(0, 1, 3, 2, 4).reshape(2, 640, 2048)


def untall(a):
    return a.reshape(2, 256, 5, 8, 128).transpose(0, 1, 3, 2, 4).reshape(2, 2048, 640)


def unwide_small(a):
    return a.reshape(5, 16, 2, 128).transpose(0, 2, 1, 3).reshape(5, 2, 2048).transpose(1, 0, 2)


def untall_small(a):
    return a.reshape(2, 2, 5, 8, 128).transpose(0, 1, 3, 2, 4).reshape(2, 16, 640)


def solution(mesh):
    def step(*arrays):
        big, small = (wide, wide, tall), (wide_small, wide_small, tall_small)
        operands = [f(a[0]) for f, a in zip(big, arrays[:3])] + [f(a) for f, a in zip(big, arrays[3:6])]
        operands += [f(a) for f, a in zip(small * 2, arrays[6:])]
        shapes = (WIDE, WIDE, TALL)
        landing = [pltpu.VMEM((3, 2, *SHARD[weight][phase]), BF16) for phase in range(3) for weight in range(3)]
        new = pl.pallas_call(
            kernel,
            name="step",
            out_shape=[jax.ShapeDtypeStruct(s, BF16) for s in shapes] + [jax.ShapeDtypeStruct(s, F32) for s in SMALL * 2],
            in_specs=[pl.BlockSpec(memory_space=pl.ANY)] * 12,
            out_specs=[pl.BlockSpec(memory_space=pl.ANY)] * 9,
            scratch_shapes=[
                *[pltpu.VMEM(s, BF16) for s in HALF * 3],
                *landing,
                *[pltpu.VMEM(s, F32) for s in SMALL * 2],
                pltpu.VMEM((320, 128), F32),
                pltpu.VMEM((2, 2, 5, 2, 64, 128), BF16),
                pltpu.VMEM((2, 80, 128), BF16),
                pltpu.VMEM((2, 1280, 128), F32),
                *[pltpu.VMEM((8, 5, 8, 128), BF16)] * 4,
                pltpu.SemaphoreType.DMA((COPIES,)),
                pltpu.SemaphoreType.DMA((COPIES,)),
                pltpu.SemaphoreType.DMA((80,)),
            ],
            compiler_params=pltpu.CompilerParams(
                collective_id=0, has_side_effects=True, vmem_limit_bytes=44 * 1024 * 1024
            ),
        )(*operands)
        back, small_back = (unwide, unwide, untall), (unwide_small, unwide_small, untall_small)
        return tuple(f(a) for f, a in zip(back + small_back * 2, new))

    all_of, cut = P(None, None, None), P(None, "dp", None)
    return jax.shard_map(
        step,
        mesh=mesh,
        in_specs=(P(("rep", "dp"), None, None, None),) * 3 + (all_of,) * 3 + (cut,) * 6,
        out_specs=(P("rep", None, None),) * 3 + (P("rep", "dp", None),) * 6,
        check_vma=False,
    )
```

```python
import jax
import jax.numpy as jnp
from jax import lax
from jax.experimental import pallas as pl
from jax.experimental.pallas import tpu as pltpu
from jax.sharding import PartitionSpec as P

F32, BF16 = jnp.float32, jnp.bfloat16
MESH = pl.DeviceIdType.MESH
COPIES = 224
WIDE, TALL = (2, 4, 4, 5, 2, 64, 128), (2, 4, 4, 4, 2, 80, 128)
HALF = ((2, 4, 4, 5, 64, 128), (2, 4, 4, 5, 64, 128), (2, 4, 4, 4, 80, 128))
SHARD = (
    ((4, 5, 64, 128), (5, 64, 128), (5, 16, 128)),
    ((4, 5, 64, 128), (4, 5, 16, 128), (5, 16, 128)),
    ((4, 4, 80, 128), (4, 80, 128), (80, 128)),
)
AXES = (("x", "y", "z"), ("y", "z", "x"), ("z", "x", "y"))
SMALL = ((5, 32, 128), (5, 32, 128), (2, 80, 128))


def adamw(w, m, v, g):
    m = 0.9 * m + 0.1 * g
    v = 0.95 * v + 0.05 * g * g
    step = m * lax.rsqrt(v + 1e-8) + 0.1 * w
    return w - 0.02 * step, m, v


def add_into(dst, *others):
    def at(index):
        total = dst[index].astype(F32)
        for one in others:
            total = total + one[index].astype(F32)
        dst[index] = total.astype(BF16)

    lead = dst.shape[:-2]
    if len(lead) < 2:
        for i in range(lead[0] if lead else 1):
            at((i,) if lead else ())
        return

    @pl.loop(0, lead[0])
    def _(i):
        for j in range(lead[1]):
            at((i, j))


def kernel(*refs):
    grads, weights, ms, vs = (refs[i : i + 3] for i in (0, 3, 6, 9))
    outs, new_ms, new_vs = (refs[i : i + 3] for i in (12, 15, 18))
    own, other = (refs[i : i + 3] for i in (21, 24))
    landing = (refs[27:30], refs[30:33], refs[33:36])
    m_in, v_in = refs[36:39], refs[39:42]
    rows, w_block, w_down, turned, out_box, in_box, back_out, back_in, send_sems, recv_sems, local_sems = refs[42:]

    me = lax.axis_index("dp")
    core = lax.rem(me, 2)
    pos = {"z": lax.rem(me // 2, 4), "y": lax.rem(me // 8, 4), "x": me // 32}
    x, y, z = pos["x"], pos["y"], pos["z"]
    d = 2 * z + core

    def device(core=core, **moved):
        at = {**pos, **moved}
        return ((at["x"] * 4 + at["y"]) * 4 + at["z"]) * 2 + core

    def step(axis, by):
        return lax.rem(pos[axis] + by + 4, 4)

    partner = device(core=1 - core)
    right = {a: device(**{a: step(a, 1)}) for a in "xyz"}
    left = {a: device(**{a: step(a, -1)}) for a in "xyz"}
    line = [lax.rem(d + k, 8) for k in range(1, 8)]
    line_device = [device(core=lax.rem(t, 2), z=t // 2) for t in line]

    used = [0, 0]
    sent = []

    def send(src, dst, to):
        copy = pltpu.make_async_remote_copy(
            src_ref=src,
            dst_ref=dst,
            send_sem=send_sems.at[used[0]],
            recv_sem=recv_sems.at[used[0]],
            device_id={"dp": to},
            device_id_type=MESH,
        )
        used[0] += 1
        copy.start()
        sent.append(copy)
        return copy

    def local(src, dst):
        copy = pltpu.make_async_copy(src, dst, local_sems.at[used[1]])
        used[1] += 1
        copy.start()
        return copy

    def of_whole(ref, weight, layer, s, side):
        if weight == 0:
            return ref.at[layer, s, :, :, side]
        if weight == 1:
            return ref.at[layer, :, s, :, side]
        return ref.at[layer, :, :, s, side]

    def part(ref, weight, phase, layer, s):
        if phase == 0:
            return ref.at[layer, s]
        first = pos[AXES[weight][0]]
        if weight == 0:
            z = pl.ds(pl.multiple_of(16 * s, 16), 16)
            return ref.at[layer, first, s] if phase == 1 else ref.at[layer, first, pos["y"], :, z]
        if weight == 1:
            z = pl.ds(pl.multiple_of(16 * (s if phase == 1 else pos["z"]), 16), 16)
            return ref.at[layer, first, :, :, z] if phase == 1 else ref.at[layer, first, s, :, z]
        return ref.at[layer, first, s] if phase == 1 else ref.at[layer, first, pos["x"], s]

    def part_of_whole(ref, weight, phase, layer, s):
        if phase == 0:
            return of_whole(ref, weight, layer, s, core)
        if weight == 0:
            rows_of_z = pl.ds(pl.multiple_of(16 * s, 16), 16)
            return ref.at[layer, x, s, :, core] if phase == 1 else ref.at[layer, x, y, :, core, rows_of_z]
        if weight == 1:
            rows_of_z = pl.ds(pl.multiple_of(16 * (s if phase == 1 else z), 16), 16)
            return ref.at[layer, :, y, :, core, rows_of_z] if phase == 1 else ref.at[layer, s, y, :, core, rows_of_z]
        return ref.at[layer, s, :, z, core] if phase == 1 else ref.at[layer, x, s, z, core]

    order = (((2, 0), (2, 1)), ((1, 1), (-1, 0)), ((1, 0), (-1, 1)), ((0, 0), (0, 1)))
    loads = {}
    for group in order:
        for by, layer in group:
            for weight in range(3):
                s = step(AXES[weight][0], by)
                loads[weight, by, layer] = local(of_whole(grads[weight], weight, layer, s, core), own[weight].at[layer, s])
    small = [local(ms[i], m_in[i]) for i in range(3)] + [local(vs[i], v_in[i]) for i in range(3)]
    small += [local(weights[i].at[:, x, y], w_block.at[i]) for i in range(2)]
    small += [local(weights[2].at[:, x, y, z, core], w_down)]

    barrier = pltpu.get_barrier_semaphore()
    peers = [right["x"], left["x"], right["y"], left["y"], *line_device]
    for peer in peers:
        pl.semaphore_signal(barrier, inc=1, device_id={"dp": peer}, device_id_type=MESH)
    pl.semaphore_wait(barrier, len(peers))

    pairs = {}
    for group in order:
        for by, layer in group:
            for weight in range(3):
                s = step(AXES[weight][0], by)
                pairs[weight, by, layer] = send(
                    of_whole(grads[weight], weight, layer, s, 1 - core), other[weight].at[layer, s], partner
                )

    def pair_sum(weight, by, layer, *more):
        loads[weight, by, layer].wait()
        pairs[weight, by, layer].wait_recv()
        s = step(AXES[weight][0], by)
        add_into(own[weight].at[layer, s], other[weight].at[layer, s], *more)

    for phase in range(3):
        first, raw, summed = {}, {}, {}

        def shard(weight, by, layer, phase=phase):
            return part(own[weight], weight, phase, layer, step(AXES[weight][phase], by))

        def land(weight, which, layer, phase=phase):
            return landing[phase][weight].at[which, layer]

        def ways(weight, phase=phase):
            axis = AXES[weight][phase]
            return right[axis], left[axis]

        for weight in range(3):
            for layer in range(2):
                if phase == 0:
                    pair_sum(weight, 2, layer)
                first[weight, layer] = send(shard(weight, 2, layer), land(weight, 0, layer), ways(weight)[layer])
        for weight in range(3):
            for layer, by in ((1, 1), (0, -1)):
                if phase == 0:
                    pair_sum(weight, by, layer)
                raw[weight, layer] = send(shard(weight, by, layer), land(weight, 1, layer), ways(weight)[1 - layer])
        if phase == 0:
            for weight in range(3):
                for layer, by in ((0, 1), (1, -1)):
                    pair_sum(weight, by, layer)
        for weight in range(3):
            for layer, by in ((0, 1), (1, -1)):
                first[weight, layer].wait_recv()
                add_into(shard(weight, by, layer), land(weight, 0, layer))
                summed[weight, layer] = send(shard(weight, by, layer), land(weight, 2, layer), ways(weight)[layer])
        if phase == 0:
            for weight in range(3):
                for layer in range(2):
                    pair_sum(weight, 0, layer)
        if phase == 1:
            for one in small:
                one.wait()
            for weight in range(2):
                for layer in range(2):

                    @pl.loop(0, 5)
                    def _(i, weight=weight, layer=layer):
                        for side in range(2):
                            block = w_block[weight, layer, i, side].astype(F32)
                            for t in range(8):
                                start = 256 * i + 2 * (8 * side + t) + layer
                                turned[weight, pl.ds(start, 8, 32), :] = block[8 * t : 8 * t + 8]
        for weight in range(3):
            for layer in range(2):
                raw[weight, layer].wait_recv()
                summed[weight, layer].wait_recv()
                add_into(shard(weight, 0, layer), land(weight, 1, layer), land(weight, 2, layer))

    for weight in range(2):
        for layer in range(2):
            block = part(own[weight], weight, 2, layer, pos[AXES[weight][2]])
            for i in range(5):
                both = block[i].astype(F32)
                for t in range(2):
                    rows[pl.ds(64 * i + 4 * weight + 2 * t + layer, 8, 8), :] = both[8 * t : 8 * t + 8]
    for t in range(8):
        out_box[t] = rows[40 * t : 40 * t + 40].reshape(5, 8, 128).astype(BF16)
    moves = [send(out_box.at[t], in_box.at[d], to) for t, to in zip(line, line_device)]
    in_box[d] = out_box[d]

    for layer in range(2):
        g = part(own[2], 2, 2, layer, pos["y"])[...].astype(F32)
        w, m, v = adamw(w_down[layer].astype(F32), m_in[2][layer], v_in[2][layer], g)
        new_ms[2][layer] = m
        new_vs[2][layer] = v
        outs[2][layer, x, y, z, core] = w.astype(BF16)

    for one in moves:
        one.wait_recv()
    low = lax.broadcasted_iota(jnp.int32, (8, 128), 0) < 4

    def swap(a, b):
        return jnp.where(low, a, pltpu.roll(b, 4, 0)), jnp.where(low, pltpu.roll(a, 4, 0), b)

    for side in range(2):
        for half in range(2):
            even, odd = 4 * half + side, 4 * half + 2 + side

            @pl.loop(0, 5)
            def _(r, side=side, half=half, even=even, odd=odd):
                new = []
                at = 8 * (2 * side + half)
                gs = swap(in_box[even, r].astype(F32), in_box[odd, r].astype(F32))
                for weight in range(2):
                    here = (r, pl.ds(at, 8))
                    w = turned[weight, pl.ds(pl.multiple_of(160 * d + 32 * r + at, 8), 8), :]
                    w, m, v = adamw(w, m_in[weight][here], v_in[weight][here], gs[weight])
                    new_ms[weight][here] = m
                    new_vs[weight][here] = v
                    new.append(w)
                to_even, to_odd = swap(*new)
                back_out[even, r] = to_even.astype(BF16)
                back_out[odd, r] = to_odd.astype(BF16)

    moves = [send(back_out.at[t], back_in.at[d], to) for t, to in zip(line, line_device)]
    back_in[d] = back_out[d]
    for one in moves:
        one.wait_recv()
    for t in range(8):
        rows[40 * t : 40 * t + 40] = back_in[t].astype(F32).reshape(40, 128)
    for weight in range(2):
        for layer in range(2):
            block = part_of_whole(outs[weight], weight, 2, layer, pos[AXES[weight][2]])
            for i in range(5):
                both = [rows[pl.ds(64 * i + 4 * weight + 2 * t + layer, 8, 8), :] for t in range(2)]
                block[i] = jnp.concatenate(both, 0).astype(BF16)

    arrivals = []
    for phase in (2, 1, 0):
        firsts, lasts, forwards = {}, {}, {}

        def shard(weight, by, layer, phase=phase):
            return part_of_whole(outs[weight], weight, phase, layer, step(AXES[weight][phase], by))

        def spread(weight, by, layer, phase=phase):
            if phase == 0:
                arrivals.append(send(shard(weight, by, layer), shard(weight, by, layer), partner))

        for weight in range(3):
            axis = AXES[weight][phase]
            for layer in range(2):
                firsts[weight, layer] = send(shard(weight, 0, layer), shard(weight, 0, layer), (right[axis], left[axis])[layer])
        for weight in range(3):
            axis = AXES[weight][phase]
            for layer in range(2):
                lasts[weight, layer] = send(shard(weight, 0, layer), shard(weight, 0, layer), (left[axis], right[axis])[layer])
        for weight in range(3):
            for layer in range(2):
                spread(weight, 0, layer)
        for weight in range(3):
            axis = AXES[weight][phase]
            for layer, by in ((0, -1), (1, 1)):
                firsts[weight, layer].wait_recv()
                forwards[weight, layer] = send(shard(weight, by, layer), shard(weight, by, layer), (right[axis], left[axis])[layer])
                spread(weight, by, layer)
        for weight in range(3):
            for layer, by in ((0, 1), (1, -1)):
                lasts[weight, layer].wait_recv()
                spread(weight, by, layer)
        for weight in range(3):
            for layer in range(2):
                forwards[weight, layer].wait_recv()
                spread(weight, 2, layer)

    for one in arrivals:
        one.wait_recv()
    for one in sent:
        one.wait_send()


def write_out(*refs):
    copies, sems = [], refs[-1]
    for src, dst in zip(refs[:9], refs[9:18]):
        parts = [(i, j) for i in range(2) for j in range(4)] if len(src.shape) == 7 else [()]
        for at in parts:
            src_at, dst_at = (src.at[at], dst.at[at]) if at else (src, dst)
            copies.append(pltpu.make_async_copy(src_at, dst_at, sems.at[len(copies)]))
            copies[-1].start()
    for one in copies:
        one.wait()


def wide(a):
    return a.reshape(2, 80, 8, 16, 128).transpose(0, 1, 3, 2, 4).reshape(WIDE)


def tall(a):
    return a.reshape(2, 256, 8, 5, 128).transpose(0, 1, 3, 2, 4).reshape(TALL)


def wide_small(a):
    return a.transpose(1, 0, 2).reshape(5, 2, 16, 128).transpose(0, 2, 1, 3).reshape(5, 32, 128)


def tall_small(a):
    return a.reshape(2, 2, 8, 5, 128).transpose(0, 1, 3, 2, 4).reshape(2, 80, 128)


def unwide(a):
    return a.reshape(2, 80, 16, 8, 128).transpose(0, 1, 3, 2, 4).reshape(2, 640, 2048)


def untall(a):
    return a.reshape(2, 256, 5, 8, 128).transpose(0, 1, 3, 2, 4).reshape(2, 2048, 640)


def unwide_small(a):
    return a.reshape(5, 16, 2, 128).transpose(0, 2, 1, 3).reshape(5, 2, 2048).transpose(1, 0, 2)


def untall_small(a):
    return a.reshape(2, 2, 5, 8, 128).transpose(0, 1, 3, 2, 4).reshape(2, 16, 640)


def solution(mesh):
    def step(*arrays):
        big, small = (wide, wide, tall), (wide_small, wide_small, tall_small)
        operands = [f(a[0]) for f, a in zip(big, arrays[:3])] + [f(a) for f, a in zip(big, arrays[3:6])]
        operands += [f(a) for f, a in zip(small * 2, arrays[6:])]
        shapes = (WIDE, WIDE, TALL)
        landing = [pltpu.VMEM((3, 2, *SHARD[weight][phase]), BF16) for phase in range(3) for weight in range(3)]
        results = [(s, BF16) for s in shapes] + [(s, F32) for s in SMALL * 2]
        new = pl.pallas_call(
            kernel,
            name="step",
            out_shape=[pltpu.VMEM(s, t) for s, t in results],
            in_specs=[pl.BlockSpec(memory_space=pltpu.HBM)] * 12,
            out_specs=[pl.BlockSpec(memory_space=pltpu.VMEM)] * 9,
            scratch_shapes=[
                *[pltpu.VMEM(s, BF16) for s in HALF * 2],
                *landing,
                *[pltpu.VMEM(s, F32) for s in SMALL * 2],
                pltpu.VMEM((320, 128), F32),
                pltpu.VMEM((2, 2, 5, 2, 64, 128), BF16),
                pltpu.VMEM((2, 80, 128), BF16),
                pltpu.VMEM((2, 1280, 128), F32),
                *[pltpu.VMEM((8, 5, 8, 128), BF16)] * 4,
                pltpu.SemaphoreType.DMA((COPIES,)),
                pltpu.SemaphoreType.DMA((COPIES,)),
                pltpu.SemaphoreType.DMA((80,)),
            ],
            compiler_params=pltpu.CompilerParams(
                collective_id=0, has_side_effects=True, vmem_limit_bytes=44 * 1024 * 1024
            ),
        )(*operands)
        new = pl.pallas_call(
            write_out,
            name="write_out",
            out_shape=[jax.ShapeDtypeStruct(s, t) for s, t in results],
            in_specs=[pl.BlockSpec(memory_space=pl.ANY)] * 9,
            out_specs=[pl.BlockSpec(memory_space=pltpu.HBM)] * 9,
            scratch_shapes=[pltpu.SemaphoreType.DMA((30,))],
            compiler_params=pltpu.CompilerParams(vmem_limit_bytes=1024 * 1024),
        )(*new)
        back, small_back = (unwide, unwide, untall), (unwide_small, unwide_small, untall_small)
        return tuple(f(a) for f, a in zip(back + small_back * 2, new))

    all_of, cut = P(None, None, None), P(None, "dp", None)
    return jax.shard_map(
        step,
        mesh=mesh,
        in_specs=(P(("rep", "dp"), None, None, None),) * 3 + (all_of,) * 3 + (cut,) * 6,
        out_specs=(P("rep", None, None),) * 3 + (P("rep", "dp", None),) * 6,
        check_vma=False,
    )
```

```python
import jax
import jax.numpy as jnp
from jax import lax
from jax.experimental import pallas as pl
from jax.experimental.pallas import tpu as pltpu
from jax.sharding import PartitionSpec as P

F32, BF16 = jnp.float32, jnp.bfloat16
MESH = pl.DeviceIdType.MESH
ALL = slice(None)
ROW = 128
WIDE, TALL = (2, 4, 4, 5, 2, 64, ROW), (2, 4, 4, 4, 2, 80, ROW)
HALF = (*[(2, 4, 4, 5, 64, ROW)] * 2, (2, 4, 4, 4, 80, ROW))
AXES = (("xyz", "xyz"), ("yxz", "yxz"), ("zxy", "zyx"))
CUT = (("yz", "yz"), ("xz", "xz"), ("xy", "xx"))
PIECE = ((*[(2, 5, 64, ROW)] * 2, (2, 4, 80, ROW)), (*[(5, 32, ROW)] * 2, (2, 80, ROW)))
SMALL = (*[(160, ROW)] * 2, (2, 80, ROW))
BOX = (2, 5, 8, ROW)
SENDS, RECVS, LOCALS, LAG = 110, 160, 28, 14
ORDER = (
    "A0 R0 O0 B0",
    "W0 A1 C0 R1",
    "O1 W1 D0 B1",
    "E0 C1 H0 D1",
    "J0 E1 K0 H1",
    "L0 J1 Q0 M0",
    "K1 L1 Q1 N0",
    "M1 N1",
)


def adamw(w, m, v, g):
    m = 0.9 * m + 0.1 * g
    v = 0.95 * v + 0.05 * g * g
    step = m * lax.rsqrt(v + 1e-8) + 0.1 * w
    return w - 0.02 * step, m, v


def add_into(dst, *others):
    def at(*index):
        total = dst[index].astype(F32)
        for one in others:
            total = total + one[index].astype(F32)
        dst[index] = total.astype(BF16)

    lead = dst.shape[:-2]
    if not lead:
        at()
    elif len(lead) == 1:
        for i in range(lead[0]):
            at(i)
    else:

        @pl.loop(0, lead[0])
        def _(i):
            for j in range(lead[1]):
                at(i, j)


def kernel(*refs):
    refs = list(refs)

    def take(n):
        taken = refs[:n]
        del refs[:n]
        return taken

    grads, weights, ms, vs, outs, new_ms, new_vs, own, other, *landing, m_in, v_in = (take(3) for _ in range(13))
    last_landing = refs.pop(0)
    w_block, w_down, turned, spread, out_box, in_box, back_out, back_in, send_sems, recv_sems, local_sems = refs

    me = lax.axis_index("dp")
    core = lax.rem(me, 2)
    pos = {"z": lax.rem(lax.div(me, 2), 4), "y": lax.rem(lax.div(me, 8), 4), "x": lax.div(me, 32)}
    x, y, z = (pos[a] for a in "xyz")
    d = 2 * z + core

    stride = {"x": 32, "y": 8, "z": 2}
    steps = {(a, by): lax.rem(pos[a] + by, 4) if by else pos[a] for a in "xyz" for by in (0, 1, 2, 3)}
    devices = {(a, by): me + stride[a] * (steps[a, by] - pos[a]) for a in "xyz" for by in (1, 2, 3)}
    z_rows = [pl.multiple_of(16 * steps["z", by], 16) for by in range(4)]

    def step(axis, by):
        return steps[axis, by % 4]

    def to(axis, by):
        return devices[axis, by % 4]

    partner = me + 1 - 2 * core
    line = [lax.rem(d + i, 8) for i in range(1, 8)]
    line_device = [me - d + t for t in line]
    locals_ = []

    copies, leaving, free_sends, used = {}, [[]], list(range(SENDS)), [0]

    def recycle(stages=LAG):
        leaving.append([])
        for copy, n in (one for old in leaving[:-stages] for one in old):
            copy.wait_send()
            free_sends.append(n)
        del leaving[:-stages]

    def send(src, dst, device_id, key, recv_sem=None):
        if recv_sem is None:
            recv_sem = used[0]
            used[0] += 1
        n = free_sends.pop(0)
        copy = pltpu.make_async_remote_copy(
            src_ref=src,
            dst_ref=dst,
            send_sem=send_sems.at[n],
            recv_sem=recv_sems.at[recv_sem],
            device_id={"dp": device_id},
            device_id_type=MESH,
        )
        copy.start()
        leaving[-1].append((copy, n))
        copies.setdefault(key, []).append(copy)
        return recv_sem

    def arrived(*key):
        for copy in copies[key]:
            copy.wait_recv()

    recv_of = {}

    def local(src, dst, *key):
        copy = pltpu.make_async_copy(src, dst, local_sems.at[len(locals_)])
        copy.start()
        locals_.append(copy)
        return copy

    def spot(w, phase, k, by, half):
        at = {}
        for p, axis in enumerate(AXES[w][k]):
            at[axis] = pos[axis] if p < phase else step(axis, by) if p == phase else ALL
        p = AXES[w][k].index("z")
        rows = ALL if p > phase else pl.ds(z_rows[by % 4 if p == phase else 0], 16)
        if half is not None:
            at[CUT[w][k][phase]] = pl.ds(2 * half, 2)
            if CUT[w][k][phase] == "z":
                rows = pl.ds(32 * half, 32)
        return at["x"], at["y"], at["z"], rows

    def mine(w, phase, k, by, half=None):
        sx, sy, sz, rows = spot(w, phase, k, by, half)
        if w == 2:
            return own[w].at[k, sz, sx, sy]
        first, second = (sx, sy) if w == 0 else (sy, sx)
        return own[w].at[k, first, second, :, rows]

    def whole(ref, w, phase, k, by, half=None, side=core):
        sx, sy, sz, rows = spot(w, phase, k, by, half)
        return ref.at[k, sx, sy, sz, side] if w == 2 else ref.at[k, sx, sy, :, side, rows]

    shards = (2, 1, -1, 0)
    loads = {}
    for k in range(2):
        for by in shards:
            for w in range(3):
                if w == 0 and by == 2:
                    loads[w, k, by] = local(grads[w].at[k, :, :, :, core], own[w].at[k], w, k, by)
                elif w:
                    loads[w, k, by] = local(whole(grads[w], w, 0, k, by), mine(w, 0, k, by), w, k, by)
    small = []
    for w in range(3):
        small += [local(ms[w], m_in[w], "m", w), local(vs[w], v_in[w], "v", w)]
    for w in range(2):
        small += [local(weights[w].at[:, x, y], w_block.at[w], "w", w)]
    small += [local(weights[2].at[:, x, y, z, core], w_down, "w", 2)]

    barrier = pltpu.get_barrier_semaphore()
    peers = [to("x", 1), to("x", -1), to("y", 1), to("y", -1), *line_device]
    for peer in peers:
        pl.semaphore_signal(barrier, inc=1, device_id={"dp": peer}, device_id_type=MESH)
    pl.semaphore_wait(barrier, len(peers))
    for k in range(2):
        for by in shards:
            for w in range(3):
                src = whole(grads[w], w, 0, k, by, side=1 - core)
                send(src, other[w].at[k, step(AXES[w][0][0], by)], partner, ("pair", w, k, by))

    def pair_sum(w, k, by):
        if w or by == 2:
            loads[w, k, by].wait()
        there = other[w].at[k, step(AXES[w][0][0], by)]
        arrived("pair", w, k, by)
        add_into(mine(w, 0, k, by), there)

    def reduce_send(w, p, k, by, which, half, way):
        key = ("r", w, p, k, 2) if which else ("r", w, p, k, 0, half)
        dst = landing[p][w].at[k, which, half]
        recv_of[w, p, k, which, half] = send(mine(w, p, k, by, half), dst, to(AXES[w][k][p], way), key)

    def open_phase(w, p, k, before=lambda w, k, by: None):
        before(w, k, 2)
        for half, way in ((0, 1), (1, -1)):
            reduce_send(w, p, k, 2, 0, half, way)

    def raw_phase(w, p, k, before=lambda w, k, by: None):
        for half, by in ((1, 1), (0, -1)):
            before(w, k, by)
            reduce_send(w, p, k, by, 1, half, by)

    def meet(w, p, k):
        for half, by in ((0, 1), (1, -1)):
            arrived("r", w, p, k, 0, half)
            add_into(mine(w, p, k, by, half), landing[p][w].at[k, 0, half])
            reduce_send(w, p, k, by, 2, half, by)

    def close(w, p, k):
        arrived("r", w, p, k, 2)
        for half in range(2):
            add_into(mine(w, p, k, 0, half), landing[p][w].at[k, 1, half], landing[p][w].at[k, 2, half])

    def stage_a(k):
        for w in range(3):
            open_phase(w, 0, k, pair_sum)

    def stage_r(k):
        for w in range(3):
            raw_phase(w, 0, k, pair_sum)

    def stage_o(k):
        for w in range(3):
            pair_sum(w, k, 0)

    def stage_b(k):
        for w in range(3):
            meet(w, 0, k)

    def stage_c(k):
        for w in range(3):
            close(w, 0, k)
            open_phase(w, 1, k)
            raw_phase(w, 1, k)

    def stage_d(k):
        for w in range(3):
            meet(w, 1, k)

    def to_line(src, dst, *key):
        for t, device_id in zip(line, line_device):
            send(src(t), dst, device_id, key)

    def stage_e(k):
        for w in range(3):
            close(w, 1, k)
            if w == 2:
                for i, by in enumerate((2, 1, -1)):
                    send(mine(w, 2, k, by), last_landing.at[k, i], to(AXES[w][k][2], by), ("r", w, 2, k))

        @pl.loop(0, 5)
        def _(i):
            for w in range(2):
                block = own[w][k, pos[AXES[w][k][0]], pos[AXES[w][k][1]], i].astype(F32)
                for t in range(8):
                    spread[w, pl.ds(64 * i + t, 8, 8), :] = block[8 * t : 8 * t + 8]

        for t in range(8):
            for w in range(2):
                out_box[k, t, w] = spread[w, 40 * t : 40 * t + 40].reshape(5, 8, ROW).astype(BF16)
        to_line(lambda t: out_box.at[k, t], in_box.at[k, d], "out", k)
        in_box[k, d] = out_box[k, d]

    def stage_h(k):
        arrived("out", k)

        @pl.loop(0, 5)
        def _(r):
            for side in range(2):
                for w in range(2):
                    g = in_box[k, side, w, r].astype(F32)
                    for t in range(1, 4):
                        g = g + in_box[k, 2 * t + side, w, r].astype(F32)
                    g = g.astype(BF16).astype(F32)
                    here = pl.ds(32 * r + 16 * side + k, 8, 2)
                    old = turned[w, k, pl.ds(pl.multiple_of(80 * d + 16 * r + 8 * side, 8), 8), :]
                    new, new_ms[w][here, :], new_vs[w][here, :] = adamw(old, m_in[w][here, :], v_in[w][here, :], g)
                    back_out[k, side, w, r] = new.astype(BF16)

        to_line(lambda t: back_out.at[k, lax.rem(t, 2)], back_in.at[k, d], "back", k)
        back_in[k, d] = back_out[k, core]
        arrived("r", 2, 2, k)
        block = mine(2, 2, k, 0)
        add_into(block, *(last_landing.at[k, i] for i in range(3)))
        new, new_ms[2][k], new_vs[2][k] = adamw(w_down[k].astype(F32), m_in[2][k], v_in[2][k], block[...].astype(F32))
        here = whole(outs[2], 2, 2, k, 0)
        here[...] = new.astype(BF16)
        for by in (2, 1, -1):
            send(here, here, to(AXES[2][k][2], by), ("g", 2, 2, k))

    def pass_on(w, p, k, by, half, way, key):
        here = whole(outs[w], w, p, k, by, half)
        which = 2 if key == 3 else 1 if key == 2 else 0
        recv_sem = None if p else recv_of[w, 0, k, which, half]
        send(here, here, to(AXES[w][k][p], way), ("g", w, p, k, key), recv_sem)

    def to_partner(w, k, by):
        here = whole(outs[w], w, 0, k, by)
        send(here, here, partner, ("end", w), (4 * k + shards.index(by)) * 3 + w)

    def open_gather(w, p, k):
        for half, way in ((0, 1), (1, -1)):
            pass_on(w, p, k, 0, half, way, half)

    def open_whole(w, k):
        for key, way in ((0, 1), (1, -1)):
            pass_on(w, 1, k, 0, None, way, key)

    def rest_gather(w, p, k):
        for half, way in ((1, 1), (0, -1)):
            pass_on(w, p, k, 0, half, way, 2)

    def forward(w, p, k):
        for half, way in ((0, 1), (1, -1)):
            arrived("g", w, p, k, half)
            pass_on(w, p, k, -way, half, way, 3)

    def stage_j(k):
        arrived("back", k)
        for w in range(2):
            for t in range(8):
                spread[w, 40 * t : 40 * t + 40] = back_in[k, t, w].astype(F32).reshape(40, ROW)

        @pl.loop(0, 5)
        def _(i):
            for w in range(2):
                tiles = [spread[w, pl.ds(64 * i + t, 8, 8), :] for t in range(8)]
                outs[w][k, x, y, i, core] = jnp.concatenate(tiles, 0).astype(BF16)

        for w in range(2):
            open_whole(w, k)
        arrived("g", 2, 2, k)
        open_whole(2, k)

    def stage_k(k):
        for w in range(3):
            forward(w, 1, k)

    def stage_l(k):
        for w in range(3):
            arrived("g", w, 1, k, 3)
            open_gather(w, 0, k)

    def stage_q(k):
        for w in range(3):
            rest_gather(w, 0, k)
            to_partner(w, k, 0)

    def stage_m(k):
        for w in range(3):
            forward(w, 0, k)

    def stage_n(k):
        for w in range(3):
            arrived("g", w, 0, k, 2)
            for by in (-1, 1):
                to_partner(w, k, by)
        for w in range(3):
            arrived("g", w, 0, k, 3)
            to_partner(w, k, 2)

    def stage_w(k):
        if k == 0:
            for one in small:
                one.wait()

        @pl.loop(0, 5)
        def _(i):
            for w in range(2):
                for side in range(2):
                    block = w_block[w, k, i, side].astype(F32)
                    for t in range(8):
                        turned[w, k, pl.ds(128 * i + 8 * side + t, 8, 16), :] = block[8 * t : 8 * t + 8]

    stages = {n[6:]: f for n, f in locals().items() if n.startswith("stage_")}
    for name in " ".join(ORDER).lower().split():
        recycle()
        stages[name[0]](int(name[1]))

    for w in range(3):
        arrived("end", w)
    for copy, _ in (one for old in leaving for one in old):
        copy.wait_send()


def write_out(*refs):
    copies, sems = [], refs[-1]
    for src, dst in zip(refs[:9], refs[9:18]):
        for at in [(i, j) for i in range(2) for j in range(4)] if len(src.shape) == 7 else [(ALL,)]:
            copies.append(pltpu.make_async_copy(src.at[at], dst.at[at], sems.at[len(copies)]))
            copies[-1].start()
    for one in copies:
        one.wait()


SWAP = (0, 1, 3, 2, 4)


def wide(a):
    return a.reshape(2, 80, 8, 16, ROW).transpose(SWAP).reshape(WIDE)


def tall(a):
    return a.reshape(2, 256, 8, 5, ROW).transpose(SWAP).reshape(TALL)


def wide_small(a):
    return a.reshape(2, 5, 16, ROW).transpose(1, 2, 0, 3).reshape(SMALL[0])


def tall_small(a):
    return a.reshape(2, 2, 8, 5, ROW).transpose(SWAP).reshape(SMALL[2])


def unwide(a):
    return a.reshape(2, 80, 16, 8, ROW).transpose(SWAP).reshape(2, 640, 2048)


def untall(a):
    return a.reshape(2, 256, 5, 8, ROW).transpose(SWAP).reshape(2, 2048, 640)


def unwide_small(a):
    return a.reshape(5, 16, 2, ROW).transpose(2, 0, 1, 3).reshape(2, 5, 2048)


def untall_small(a):
    return a.reshape(2, 2, 5, 8, ROW).transpose(SWAP).reshape(2, 16, 640)


def solution(mesh):
    def step(*arrays):
        big, small = (wide, wide, tall), (wide_small, wide_small, tall_small)
        operands = [f(a[0]) for f, a in zip(big, arrays)] + [f(a) for f, a in zip(big + small * 2, arrays[3:])]
        results = [(s, BF16) for s in (WIDE, WIDE, TALL)] + [(s, F32) for s in SMALL * 2]
        new = pl.pallas_call(
            kernel,
            name="step",
            out_shape=[pltpu.VMEM(s, t) for s, t in results],
            in_specs=[pl.BlockSpec(memory_space=pltpu.HBM)] * 12,
            out_specs=[pl.BlockSpec(memory_space=pltpu.VMEM)] * 9,
            scratch_shapes=[
                *[pltpu.VMEM(s, BF16) for s in HALF * 2],
                *[pltpu.VMEM((2, 3, 2, *s), BF16) for p in PIECE for s in p],
                *[pltpu.VMEM(s, F32) for s in SMALL * 2],
                pltpu.VMEM((2, 3, 80, ROW), BF16),
                pltpu.VMEM((2, 2, 5, 2, 64, ROW), BF16),
                pltpu.VMEM(SMALL[2], BF16),
                pltpu.VMEM((2, 2, 640, ROW), F32),
                pltpu.VMEM((2, 320, ROW), F32),
                *[pltpu.VMEM((2, n, *BOX), BF16) for n in (8, 8, 2, 8)],
                *[pltpu.SemaphoreType.DMA((n,)) for n in (SENDS, RECVS, LOCALS)],
            ],
            compiler_params=pltpu.CompilerParams(collective_id=0, has_side_effects=True, vmem_limit_bytes=44 << 20),
        )(*operands)
        new = pl.pallas_call(
            write_out,
            name="write_out",
            out_shape=[jax.ShapeDtypeStruct(s, t) for s, t in results],
            in_specs=[pl.BlockSpec(memory_space=pl.ANY)] * 9,
            out_specs=[pl.BlockSpec(memory_space=pltpu.HBM)] * 9,
            scratch_shapes=[pltpu.SemaphoreType.DMA((30,))],
            compiler_params=pltpu.CompilerParams(vmem_limit_bytes=1 << 20),
        )(*new)
        back, small_back = (unwide, unwide, untall), (unwide_small, unwide_small, untall_small)
        return tuple(f(a) for f, a in zip(back + small_back * 2, new))

    all_of, cut = P(None, None, None), P(None, "dp", None)
    return jax.shard_map(
        step,
        mesh=mesh,
        in_specs=(P(("rep", "dp"), None, None, None),) * 3 + (all_of,) * 3 + (cut,) * 6,
        out_specs=(P("rep", None, None),) * 3 + (P("rep", "dp", None),) * 6,
        check_vma=False,
    )
```

```python
import jax
import jax.numpy as jnp
from jax import lax
from jax.experimental import pallas as pl
from jax.experimental.pallas import tpu as pltpu
from jax.sharding import PartitionSpec as P

F32, BF16 = jnp.float32, jnp.bfloat16
MESH = pl.DeviceIdType.MESH
ALL = slice(None)
ROW = 128
WIDE, TALL = (2, 4, 4, 5, 2, 64, ROW), (2, 4, 4, 4, 2, 80, ROW)
HALF = (*[(2, 4, 4, 5, 64, ROW)] * 2, (2, 4, 4, 4, 80, ROW))
AXES = (("xyz", "xyz"), ("yxz", "yxz"), ("zxy", "zyx"))
CUT = (("yz", "yz"), ("xz", "xz"), ("xy", "xx"))
PIECE = ((*[(2, 5, 64, ROW)] * 2, (2, 4, 80, ROW)), (*[(5, 32, ROW)] * 2, (2, 80, ROW)))
SMALL = (*[(160, ROW)] * 2, (2, 80, ROW))
BOX = (2, 5, 8, ROW)
SENDS, RECVS, LOCALS, LAG = 70, 160, 28, 8
ORDER = (
    "A0 R0 O0 B0",
    "W0 A1 C0 R1",
    "O1 W1 D0 B1",
    "E0 C1 H0 D1",
    "J0 E1 K0 H1",
    "L0 Q0 J1 K1",
    "M0 L1 Q1 N0",
    "M1 N1",
)


def adamw(w, m, v, g):
    m = 0.9 * m + 0.1 * g
    v = 0.95 * v + 0.05 * g * g
    step = m * lax.rsqrt(v + 1e-8) + 0.1 * w
    return w - 0.02 * step, m, v


def add_into(dst, *others):
    def at(*index):
        total = dst[index].astype(F32)
        for one in others:
            total = total + one[index].astype(F32)
        dst[index] = total.astype(BF16)

    lead = dst.shape[:-2]
    if not lead:
        at()
    elif len(lead) == 1:
        for i in range(lead[0]):
            at(i)
    else:

        @pl.loop(0, lead[0])
        def _(i):
            for j in range(lead[1]):
                at(i, j)


def kernel(*refs):
    refs = list(refs)

    def take(n):
        taken = refs[:n]
        del refs[:n]
        return taken

    grads, weights, ms, vs, outs, new_ms, new_vs, own, other, *landing, m_in, v_in = (take(3) for _ in range(13))
    last_landing = refs.pop(0)
    w_block, w_down, turned, spread, out_box, in_box, back_out, back_in, send_sems, recv_sems, local_sems = refs

    me = lax.axis_index("dp")
    core = lax.rem(me, 2)
    pos = {"z": lax.rem(lax.div(me, 2), 4), "y": lax.rem(lax.div(me, 8), 4), "x": lax.div(me, 32)}
    x, y, z = (pos[a] for a in "xyz")
    d = 2 * z + core

    stride = {"x": 32, "y": 8, "z": 2}
    steps = {(a, by): lax.rem(pos[a] + by, 4) if by else pos[a] for a in "xyz" for by in (0, 1, 2, 3)}
    devices = {(a, by): me + stride[a] * (steps[a, by] - pos[a]) for a in "xyz" for by in (1, 2, 3)}
    z_rows = [pl.multiple_of(16 * steps["z", by], 16) for by in range(4)]

    def step(axis, by):
        return steps[axis, by % 4]

    def to(axis, by):
        return devices[axis, by % 4]

    partner = me + 1 - 2 * core
    line = [lax.rem(d + i, 8) for i in range(1, 8)]
    line_device = [me - d + t for t in line]
    locals_ = []

    copies, leaving, free_sends, used = {}, [[]], list(range(SENDS)), [0]

    def recycle(stages=LAG):
        leaving.append([])
        for copy, n in (one for old in leaving[:-stages] for one in old):
            copy.wait_send()
            free_sends.append(n)
        del leaving[:-stages]

    def send(src, dst, device_id, key, recv_sem=None):
        if recv_sem is None:
            recv_sem = used[0]
            used[0] += 1
        n = free_sends.pop(0)
        copy = pltpu.make_async_remote_copy(
            src_ref=src,
            dst_ref=dst,
            send_sem=send_sems.at[n],
            recv_sem=recv_sems.at[recv_sem],
            device_id={"dp": device_id},
            device_id_type=MESH,
        )
        copy.start()
        leaving[-1].append((copy, n))
        copies.setdefault(key, []).append(copy)
        return recv_sem

    def arrived(*key):
        for copy in copies[key]:
            copy.wait_recv()

    recv_of = {}

    def local(src, dst, *key):
        copy = pltpu.make_async_copy(src, dst, local_sems.at[len(locals_)])
        copy.start()
        locals_.append(copy)
        return copy

    def spot(w, phase, k, by, half):
        at = {}
        for p, axis in enumerate(AXES[w][k]):
            at[axis] = pos[axis] if p < phase else step(axis, by) if p == phase else ALL
        p = AXES[w][k].index("z")
        rows = ALL if p > phase else pl.ds(z_rows[by % 4 if p == phase else 0], 16)
        if half is not None:
            at[CUT[w][k][phase]] = pl.ds(2 * half, 2)
            if CUT[w][k][phase] == "z":
                rows = pl.ds(32 * half, 32)
        return at["x"], at["y"], at["z"], rows

    def mine(w, phase, k, by, half=None):
        sx, sy, sz, rows = spot(w, phase, k, by, half)
        if w == 2:
            return own[w].at[k, sz, sx, sy]
        first, second = (sx, sy) if w == 0 else (sy, sx)
        return own[w].at[k, first, second, :, rows]

    def whole(ref, w, phase, k, by, half=None, side=core):
        sx, sy, sz, rows = spot(w, phase, k, by, half)
        return ref.at[k, sx, sy, sz, side] if w == 2 else ref.at[k, sx, sy, :, side, rows]

    shards = (2, 1, -1, 0)
    loads = {}
    for k in range(2):
        for by in shards:
            for w in range(3):
                if w == 0 and by == 2:
                    loads[w, k, by] = local(grads[w].at[k, :, :, :, core], own[w].at[k], w, k, by)
                elif w:
                    loads[w, k, by] = local(whole(grads[w], w, 0, k, by), mine(w, 0, k, by), w, k, by)
    small = []
    for w in range(3):
        small += [local(ms[w], m_in[w], "m", w), local(vs[w], v_in[w], "v", w)]
    for w in range(2):
        small += [local(weights[w].at[:, x, y], w_block.at[w], "w", w)]
    small += [local(weights[2].at[:, x, y, z, core], w_down, "w", 2)]

    barrier = pltpu.get_barrier_semaphore()
    peers = [to("x", 1), to("x", -1), to("y", 1), to("y", -1), *line_device]
    for peer in peers:
        pl.semaphore_signal(barrier, inc=1, device_id={"dp": peer}, device_id_type=MESH)
    pl.semaphore_wait(barrier, len(peers))
    for k in range(2):
        for by in shards:
            for w in range(3):
                src = whole(grads[w], w, 0, k, by, side=1 - core)
                send(src, other[w].at[k, step(AXES[w][0][0], by)], partner, ("pair", w, k, by))

    def pair_sum(w, k, by):
        if w or by == 2:
            loads[w, k, by].wait()
        there = other[w].at[k, step(AXES[w][0][0], by)]
        arrived("pair", w, k, by)
        add_into(mine(w, 0, k, by), there)

    def reduce_send(w, p, k, by, which, half, way):
        key = ("r", w, p, k, 2) if which else ("r", w, p, k, 0, half)
        dst = landing[p][w].at[k, which, half]
        recv_of[w, p, k, which, half] = send(mine(w, p, k, by, half), dst, to(AXES[w][k][p], way), key)

    def open_phase(w, p, k, before=lambda w, k, by: None):
        before(w, k, 2)
        for half, way in ((0, 1), (1, -1)):
            reduce_send(w, p, k, 2, 0, half, way)

    def raw_phase(w, p, k, before=lambda w, k, by: None):
        for half, by in ((1, 1), (0, -1)):
            before(w, k, by)
            reduce_send(w, p, k, by, 1, half, by)

    def meet(w, p, k):
        for half, by in ((0, 1), (1, -1)):
            arrived("r", w, p, k, 0, half)
            add_into(mine(w, p, k, by, half), landing[p][w].at[k, 0, half])
            reduce_send(w, p, k, by, 2, half, by)

    def close(w, p, k):
        arrived("r", w, p, k, 2)
        for half in range(2):
            add_into(mine(w, p, k, 0, half), landing[p][w].at[k, 1, half], landing[p][w].at[k, 2, half])

    def stage_a(k):
        for w in range(3):
            open_phase(w, 0, k, pair_sum)

    def stage_r(k):
        for w in range(3):
            raw_phase(w, 0, k, pair_sum)

    def stage_o(k):
        for w in range(3):
            pair_sum(w, k, 0)

    def stage_b(k):
        for w in range(3):
            meet(w, 0, k)

    def stage_c(k):
        for w in range(3):
            close(w, 0, k)
            open_phase(w, 1, k)
            raw_phase(w, 1, k)

    def stage_d(k):
        for w in range(3):
            meet(w, 1, k)

    def to_line(src, dst, *key):
        for t, device_id in zip(line, line_device):
            send(src(t), dst, device_id, key)

    def stage_e(k):
        for w in range(3):
            close(w, 1, k)
            if w == 2:
                for i, by in enumerate((2, 1, -1)):
                    send(mine(w, 2, k, by), last_landing.at[k, i], to(AXES[w][k][2], by), ("r", w, 2, k))

        @pl.loop(0, 5)
        def _(i):
            for w in range(2):
                block = own[w][k, pos[AXES[w][k][0]], pos[AXES[w][k][1]], i].astype(F32)
                for t in range(8):
                    spread[w, pl.ds(64 * i + t, 8, 8), :] = block[8 * t : 8 * t + 8]

        for t in range(8):
            for w in range(2):
                out_box[k, t, w] = spread[w, 40 * t : 40 * t + 40].reshape(5, 8, ROW).astype(BF16)
        to_line(lambda t: out_box.at[k, t], in_box.at[k, d], "out", k)
        in_box[k, d] = out_box[k, d]

    def stage_h(k):
        arrived("out", k)

        @pl.loop(0, 5)
        def _(r):
            for side in range(2):
                for w in range(2):
                    g = in_box[k, side, w, r].astype(F32)
                    for t in range(1, 4):
                        g = g + in_box[k, 2 * t + side, w, r].astype(F32)
                    g = g.astype(BF16).astype(F32)
                    here = pl.ds(32 * r + 16 * side + k, 8, 2)
                    old = turned[w, k, pl.ds(pl.multiple_of(80 * d + 16 * r + 8 * side, 8), 8), :]
                    new, new_ms[w][here, :], new_vs[w][here, :] = adamw(old, m_in[w][here, :], v_in[w][here, :], g)
                    back_out[k, side, w, r] = new.astype(BF16)

        to_line(lambda t: back_out.at[k, lax.rem(t, 2)], back_in.at[k, d], "back", k)
        back_in[k, d] = back_out[k, core]
        arrived("r", 2, 2, k)
        block = mine(2, 2, k, 0)
        add_into(block, *(last_landing.at[k, i] for i in range(3)))
        new, new_ms[2][k], new_vs[2][k] = adamw(w_down[k].astype(F32), m_in[2][k], v_in[2][k], block[...].astype(F32))
        here = whole(outs[2], 2, 2, k, 0)
        here[...] = new.astype(BF16)
        for by in (2, 1, -1):
            send(here, here, to(AXES[2][k][2], by), ("g", 2, 2, k))

    def pass_on(w, p, k, by, half, way, key):
        here = whole(outs[w], w, p, k, by, half)
        which = 2 if key == 3 else 1 if key == 2 else 0
        recv_sem = None if p else recv_of[w, 0, k, which, half]
        send(here, here, to(AXES[w][k][p], way), ("g", w, p, k, key), recv_sem)

    def to_partner(w, k, by):
        here = whole(outs[w], w, 0, k, by)
        send(here, here, partner, ("end", w), (4 * k + shards.index(by)) * 3 + w)

    def open_gather(w, p, k):
        for half, way in ((0, 1), (1, -1)):
            pass_on(w, p, k, 0, half, way, half)

    def open_whole(w, k):
        for key, way in ((0, 1), (1, -1)):
            pass_on(w, 1, k, 0, None, way, key)

    def rest_gather(w, p, k):
        for half, way in ((1, 1), (0, -1)):
            pass_on(w, p, k, 0, half, way, 2)

    def forward(w, p, k):
        for half, way in ((0, 1), (1, -1)):
            arrived("g", w, p, k, half)
            pass_on(w, p, k, -way, half, way, 3)

    def stage_j(k):
        arrived("back", k)
        for w in range(2):
            for t in range(8):
                spread[w, 40 * t : 40 * t + 40] = back_in[k, t, w].astype(F32).reshape(40, ROW)

        @pl.loop(0, 5)
        def _(i):
            for w in range(2):
                tiles = [spread[w, pl.ds(64 * i + t, 8, 8), :] for t in range(8)]
                outs[w][k, x, y, i, core] = jnp.concatenate(tiles, 0).astype(BF16)

        for w in range(2):
            open_whole(w, k)
        arrived("g", 2, 2, k)
        open_whole(2, k)

    def stage_k(k):
        for w in range(3):
            forward(w, 1, k)

    def stage_l(k):
        for w in range(3):
            arrived("g", w, 1, k, 3)
            open_gather(w, 0, k)

    def stage_q(k):
        for w in range(3):
            rest_gather(w, 0, k)
            to_partner(w, k, 0)

    def stage_m(k):
        for w in range(3):
            forward(w, 0, k)

    def stage_n(k):
        for w in range(3):
            arrived("g", w, 0, k, 2)
            for by in (-1, 1):
                to_partner(w, k, by)
        for w in range(3):
            arrived("g", w, 0, k, 3)
            to_partner(w, k, 2)

    def stage_w(k):
        if k == 0:
            for one in small:
                one.wait()

        @pl.loop(0, 5)
        def _(i):
            for w in range(2):
                for side in range(2):
                    block = w_block[w, k, i, side].astype(F32)
                    for t in range(8):
                        turned[w, k, pl.ds(128 * i + 8 * side + t, 8, 16), :] = block[8 * t : 8 * t + 8]

    stages = {n[6:]: f for n, f in locals().items() if n.startswith("stage_")}
    for i, name in enumerate(" ".join(ORDER).lower().split()):
        recycle(LAG if i < 27 else LAG // 2)
        stages[name[0]](int(name[1]))

    recycle(2)
    for w in range(3):
        arrived("end", w)
    for copy, _ in (one for old in leaving for one in old):
        copy.wait_send()


def write_out(*refs):
    copies, sems = [], refs[-1]
    for src, dst in zip(refs[:9], refs[9:18]):
        for at in [(i, j) for i in range(2) for j in range(4)] if len(src.shape) == 7 else [(ALL,)]:
            copies.append(pltpu.make_async_copy(src.at[at], dst.at[at], sems.at[len(copies)]))
            copies[-1].start()
    for one in copies:
        one.wait()


SWAP = (0, 1, 3, 2, 4)


def wide(a):
    return a.reshape(2, 80, 8, 16, ROW).transpose(SWAP).reshape(WIDE)


def tall(a):
    return a.reshape(2, 256, 8, 5, ROW).transpose(SWAP).reshape(TALL)


def wide_small(a):
    return a.reshape(2, 5, 16, ROW).transpose(1, 2, 0, 3).reshape(SMALL[0])


def tall_small(a):
    return a.reshape(2, 2, 8, 5, ROW).transpose(SWAP).reshape(SMALL[2])


def unwide(a):
    return a.reshape(2, 80, 16, 8, ROW).transpose(SWAP).reshape(2, 640, 2048)


def untall(a):
    return a.reshape(2, 256, 5, 8, ROW).transpose(SWAP).reshape(2, 2048, 640)


def unwide_small(a):
    return a.reshape(5, 16, 2, ROW).transpose(2, 0, 1, 3).reshape(2, 5, 2048)


def untall_small(a):
    return a.reshape(2, 2, 5, 8, ROW).transpose(SWAP).reshape(2, 16, 640)


def solution(mesh):
    def step(*arrays):
        big, small = (wide, wide, tall), (wide_small, wide_small, tall_small)
        operands = [f(a[0]) for f, a in zip(big, arrays)] + [f(a) for f, a in zip(big + small * 2, arrays[3:])]
        results = [(s, BF16) for s in (WIDE, WIDE, TALL)] + [(s, F32) for s in SMALL * 2]
        new = pl.pallas_call(
            kernel,
            name="step",
            out_shape=[pltpu.VMEM(s, t) for s, t in results],
            in_specs=[pl.BlockSpec(memory_space=pltpu.HBM)] * 12,
            out_specs=[pl.BlockSpec(memory_space=pltpu.VMEM)] * 9,
            scratch_shapes=[
                *[pltpu.VMEM(s, BF16) for s in HALF * 2],
                *[pltpu.VMEM((2, 3, 2, *s), BF16) for p in PIECE for s in p],
                *[pltpu.VMEM(s, F32) for s in SMALL * 2],
                pltpu.VMEM((2, 3, 80, ROW), BF16),
                pltpu.VMEM((2, 2, 5, 2, 64, ROW), BF16),
                pltpu.VMEM(SMALL[2], BF16),
                pltpu.VMEM((2, 2, 640, ROW), F32),
                pltpu.VMEM((2, 320, ROW), F32),
                *[pltpu.VMEM((2, n, *BOX), BF16) for n in (8, 8, 2, 8)],
                *[pltpu.SemaphoreType.DMA((n,)) for n in (SENDS, RECVS, LOCALS)],
            ],
            compiler_params=pltpu.CompilerParams(collective_id=0, has_side_effects=True, vmem_limit_bytes=44 << 20),
        )(*operands)
        new = pl.pallas_call(
            write_out,
            name="write_out",
            out_shape=[jax.ShapeDtypeStruct(s, t) for s, t in results],
            in_specs=[pl.BlockSpec(memory_space=pl.ANY)] * 9,
            out_specs=[pl.BlockSpec(memory_space=pltpu.HBM)] * 9,
            scratch_shapes=[pltpu.SemaphoreType.DMA((30,))],
            compiler_params=pltpu.CompilerParams(vmem_limit_bytes=1 << 20),
        )(*new)
        back, small_back = (unwide, unwide, untall), (unwide_small, unwide_small, untall_small)
        return tuple(f(a) for f, a in zip(back + small_back * 2, new))

    all_of, cut = P(None, None, None), P(None, "dp", None)
    return jax.shard_map(
        step,
        mesh=mesh,
        in_specs=(P(("rep", "dp"), None, None, None),) * 3 + (all_of,) * 3 + (cut,) * 6,
        out_specs=(P("rep", None, None),) * 3 + (P("rep", "dp", None),) * 6,
        check_vma=False,
    )
```

```python
import jax
import jax.numpy as jnp
from jax import lax
from jax.experimental import pallas as pl
from jax.experimental.pallas import tpu as pltpu
from jax.sharding import PartitionSpec as P

F32, BF16 = jnp.float32, jnp.bfloat16
MESH = pl.DeviceIdType.MESH
ALL = slice(None)
ROW = 128
WIDE, TALL = (2, 4, 4, 5, 2, 64, ROW), (2, 4, 4, 4, 2, 80, ROW)
HALF = (*[(2, 4, 4, 5, 64, ROW)] * 2, (2, 4, 4, 4, 80, ROW))
AXES = (("xyz", "xyz"), ("yxz", "yxz"), ("zxy", "zyx"))
CUT = (("yz", "yz"), ("xz", "xz"), ("xy", "xx"))
PIECE = ((*[(2, 5, 64, ROW)] * 2, (2, 4, 80, ROW)), (*[(5, 32, ROW)] * 2, (2, 80, ROW)))
SMALL = (*[(160, ROW)] * 2, (2, 80, ROW))
BOX = (2, 5, 8, ROW)
SENDS, RECVS, LOCALS, LAG = 66, 160, 28, 9
ORDER = (
    "A0 R0 O0 B0",
    "W0 A1 C0 R1",
    "O1 W1 D0 V0",
    "B1 E0 C1 H0",
    "D1 J0 V1 Y0",
    "E1 K0 H1 L0",
    "Q0 J1 Y1 K1",
    "M0 L1 Q1 N0",
    "M1 N1",
)


def adamw(w, m, v, g):
    m = 0.9 * m + 0.1 * g
    v = 0.95 * v + 0.05 * g * g
    step = m * lax.rsqrt(v + 1e-8) + 0.1 * w
    return w - 0.02 * step, m, v


def add_into(dst, *others):
    def at(*index):
        total = dst[index].astype(F32)
        for one in others:
            total = total + one[index].astype(F32)
        dst[index] = total.astype(BF16)

    lead = dst.shape[:-2]
    if not lead:
        at()
    elif len(lead) == 1:
        for i in range(lead[0]):
            at(i)
    else:

        @pl.loop(0, lead[0])
        def _(i):
            for j in range(lead[1]):
                at(i, j)


def kernel(*refs):
    refs = list(refs)

    def take(n):
        taken = refs[:n]
        del refs[:n]
        return taken

    grads, weights, ms, vs, outs, new_ms, new_vs, own, other, *landing, m_in, v_in = (take(3) for _ in range(13))
    last_landing = refs.pop(0)
    w_block, w_down, turned, spread, out_box, in_box, back_out, back_in, send_sems, recv_sems, local_sems = refs

    me = lax.axis_index("dp")
    core = lax.rem(me, 2)
    pos = {"z": lax.rem(lax.div(me, 2), 4), "y": lax.rem(lax.div(me, 8), 4), "x": lax.div(me, 32)}
    x, y, z = (pos[a] for a in "xyz")
    d = 2 * z + core

    stride = {"x": 32, "y": 8, "z": 2}
    steps = {(a, by): lax.rem(pos[a] + by, 4) if by else pos[a] for a in "xyz" for by in (0, 1, 2, 3)}
    devices = {(a, by): me + stride[a] * (steps[a, by] - pos[a]) for a in "xyz" for by in (1, 2, 3)}
    z_rows = [pl.multiple_of(16 * steps["z", by], 16) for by in range(4)]

    def step(axis, by):
        return steps[axis, by % 4]

    def to(axis, by):
        return devices[axis, by % 4]

    partner = me + 1 - 2 * core
    line = [lax.rem(d + i, 8) for i in range(1, 8)]
    line_device = [me - d + t for t in line]
    locals_ = []

    copies, leaving, free_sends, used = {}, [[]], list(range(SENDS)), [0]

    def recycle(stages=LAG):
        leaving.append([])
        for copy, n in (one for old in leaving[:-stages] for one in old):
            copy.wait_send()
            free_sends.append(n)
        del leaving[:-stages]

    def send(src, dst, device_id, key, recv_sem=None):
        if recv_sem is None:
            recv_sem = used[0]
            used[0] += 1
        n = free_sends.pop(0)
        copy = pltpu.make_async_remote_copy(
            src_ref=src,
            dst_ref=dst,
            send_sem=send_sems.at[n],
            recv_sem=recv_sems.at[recv_sem],
            device_id={"dp": device_id},
            device_id_type=MESH,
        )
        copy.start()
        leaving[-1].append((copy, n))
        copies.setdefault(key, []).append(copy)
        return recv_sem

    def arrived(*key):
        for copy in copies[key]:
            copy.wait_recv()

    recv_of = {}

    def local(src, dst, *key):
        copy = pltpu.make_async_copy(src, dst, local_sems.at[len(locals_)])
        copy.start()
        locals_.append(copy)
        return copy

    def spot(w, phase, k, by, half):
        at = {}
        for p, axis in enumerate(AXES[w][k]):
            at[axis] = pos[axis] if p < phase else step(axis, by) if p == phase else ALL
        p = AXES[w][k].index("z")
        rows = ALL if p > phase else pl.ds(z_rows[by % 4 if p == phase else 0], 16)
        if half is not None:
            at[CUT[w][k][phase]] = pl.ds(2 * half, 2)
            if CUT[w][k][phase] == "z":
                rows = pl.ds(32 * half, 32)
        return at["x"], at["y"], at["z"], rows

    def mine(w, phase, k, by, half=None):
        sx, sy, sz, rows = spot(w, phase, k, by, half)
        if w == 2:
            return own[w].at[k, sz, sx, sy]
        first, second = (sx, sy) if w == 0 else (sy, sx)
        return own[w].at[k, first, second, :, rows]

    def whole(ref, w, phase, k, by, half=None, side=core):
        sx, sy, sz, rows = spot(w, phase, k, by, half)
        return ref.at[k, sx, sy, sz, side] if w == 2 else ref.at[k, sx, sy, :, side, rows]

    shards = (2, 1, -1, 0)
    loads = {}
    for k in range(2):
        for by in shards:
            for w in range(3):
                if w == 0 and by == 2:
                    loads[w, k, by] = local(grads[w].at[k, :, :, :, core], own[w].at[k], w, k, by)
                elif w:
                    loads[w, k, by] = local(whole(grads[w], w, 0, k, by), mine(w, 0, k, by), w, k, by)
    small = []
    for w in range(3):
        small += [local(ms[w], m_in[w], "m", w), local(vs[w], v_in[w], "v", w)]
    for w in range(2):
        small += [local(weights[w].at[:, x, y], w_block.at[w], "w", w)]
    small += [local(weights[2].at[:, x, y, z, core], w_down, "w", 2)]

    barrier = pltpu.get_barrier_semaphore()
    peers = [to("x", 1), to("x", -1), to("y", 1), to("y", -1), *line_device]
    for peer in peers:
        pl.semaphore_signal(barrier, inc=1, device_id={"dp": peer}, device_id_type=MESH)
    pl.semaphore_wait(barrier, len(peers))
    for k in range(2):
        for by in shards:
            for w in range(3):
                src = whole(grads[w], w, 0, k, by, side=1 - core)
                send(src, other[w].at[k, step(AXES[w][0][0], by)], partner, ("pair", w, k, by))

    def pair_sum(w, k, by):
        if w or by == 2:
            loads[w, k, by].wait()
        there = other[w].at[k, step(AXES[w][0][0], by)]
        arrived("pair", w, k, by)
        add_into(mine(w, 0, k, by), there)

    def reduce_send(w, p, k, by, which, half, way):
        key = ("r", w, p, k, 2) if which else ("r", w, p, k, 0, half)
        dst = landing[p][w].at[k, which, half]
        recv_of[w, p, k, which, half] = send(mine(w, p, k, by, half), dst, to(AXES[w][k][p], way), key)

    def open_phase(w, p, k, before=lambda w, k, by: None):
        before(w, k, 2)
        for half, way in ((0, 1), (1, -1)):
            reduce_send(w, p, k, 2, 0, half, way)

    def raw_phase(w, p, k, before=lambda w, k, by: None):
        for half, by in ((1, 1), (0, -1)):
            before(w, k, by)
            reduce_send(w, p, k, by, 1, half, by)

    def meet(w, p, k):
        for half, by in ((0, 1), (1, -1)):
            arrived("r", w, p, k, 0, half)
            add_into(mine(w, p, k, by, half), landing[p][w].at[k, 0, half])
            reduce_send(w, p, k, by, 2, half, by)

    def close(w, p, k):
        arrived("r", w, p, k, 2)
        for half in range(2):
            add_into(mine(w, p, k, 0, half), landing[p][w].at[k, 1, half], landing[p][w].at[k, 2, half])

    def stage_a(k):
        for w in range(3):
            open_phase(w, 0, k, pair_sum)

    def stage_r(k):
        for w in range(3):
            raw_phase(w, 0, k, pair_sum)

    def stage_o(k):
        for w in range(3):
            pair_sum(w, k, 0)

    def stage_b(k):
        for w in range(3):
            meet(w, 0, k)

    def stage_c(k):
        for w in range(3):
            close(w, 0, k)
            open_phase(w, 1, k)
            raw_phase(w, 1, k)

    def stage_d(k):
        for w in range(2):
            meet(w, 1, k)

    def stage_v(k):
        meet(2, 1, k)

    def to_line(src, dst, *key):
        for t, device_id in zip(line, line_device):
            send(src(t), dst, device_id, key)

    def stage_e(k):
        for w in range(3):
            close(w, 1, k)
            if w == 2:
                for i, by in enumerate((2, 1, -1)):
                    send(mine(w, 2, k, by), last_landing.at[k, i], to(AXES[w][k][2], by), ("r", w, 2, k))

        @pl.loop(0, 5)
        def _(i):
            for w in range(2):
                block = own[w][k, pos[AXES[w][k][0]], pos[AXES[w][k][1]], i].astype(F32)
                for t in range(8):
                    spread[w, pl.ds(64 * i + t, 8, 8), :] = block[8 * t : 8 * t + 8]

        for t in range(8):
            for w in range(2):
                out_box[k, t, w] = spread[w, 40 * t : 40 * t + 40].reshape(5, 8, ROW).astype(BF16)
        to_line(lambda t: out_box.at[k, t], in_box.at[k, d], "out", k)
        in_box[k, d] = out_box[k, d]

    def stage_h(k):
        arrived("out", k)

        @pl.loop(0, 5)
        def _(r):
            for side in range(2):
                for w in range(2):
                    g = in_box[k, side, w, r].astype(F32)
                    for t in range(1, 4):
                        g = g + in_box[k, 2 * t + side, w, r].astype(F32)
                    g = g.astype(BF16).astype(F32)
                    here = pl.ds(32 * r + 16 * side + k, 8, 2)
                    old = turned[w, k, pl.ds(pl.multiple_of(80 * d + 16 * r + 8 * side, 8), 8), :]
                    new, new_ms[w][here, :], new_vs[w][here, :] = adamw(old, m_in[w][here, :], v_in[w][here, :], g)
                    back_out[k, side, w, r] = new.astype(BF16)

        to_line(lambda t: back_out.at[k, lax.rem(t, 2)], back_in.at[k, d], "back", k)
        back_in[k, d] = back_out[k, core]
        arrived("r", 2, 2, k)
        block = mine(2, 2, k, 0)
        add_into(block, *(last_landing.at[k, i] for i in range(3)))
        new, new_ms[2][k], new_vs[2][k] = adamw(w_down[k].astype(F32), m_in[2][k], v_in[2][k], block[...].astype(F32))
        here = whole(outs[2], 2, 2, k, 0)
        here[...] = new.astype(BF16)
        for by in (2, 1, -1):
            send(here, here, to(AXES[2][k][2], by), ("g", 2, 2, k))

    def pass_on(w, p, k, by, half, way, key):
        here = whole(outs[w], w, p, k, by, half)
        which = 2 if key == 3 else 1 if key == 2 else 0
        recv_sem = None if p else recv_of[w, 0, k, which, half]
        send(here, here, to(AXES[w][k][p], way), ("g", w, p, k, key), recv_sem)

    def to_partner(w, k, by):
        here = whole(outs[w], w, 0, k, by)
        send(here, here, partner, ("end", w), (4 * k + shards.index(by)) * 3 + w)

    def open_gather(w, p, k):
        for half, way in ((0, 1), (1, -1)):
            pass_on(w, p, k, 0, half, way, half)

    def open_whole(w, k):
        for key, way in ((0, 1), (1, -1)):
            pass_on(w, 1, k, 0, None, way, key)

    def rest_gather(w, p, k):
        for half, way in ((1, 1), (0, -1)):
            pass_on(w, p, k, 0, half, way, 2)

    def forward(w, p, k):
        for half, way in ((0, 1), (1, -1)):
            arrived("g", w, p, k, half)
            pass_on(w, p, k, -way, half, way, 3)

    def stage_j(k):
        arrived("back", k)
        for w in range(2):
            for t in range(8):
                spread[w, 40 * t : 40 * t + 40] = back_in[k, t, w].astype(F32).reshape(40, ROW)

        @pl.loop(0, 5)
        def _(i):
            for w in range(2):
                tiles = [spread[w, pl.ds(64 * i + t, 8, 8), :] for t in range(8)]
                outs[w][k, x, y, i, core] = jnp.concatenate(tiles, 0).astype(BF16)

        for w in range(2):
            open_whole(w, k)

    def stage_y(k):
        arrived("g", 2, 2, k)
        open_whole(2, k)

    def stage_k(k):
        for w in range(3):
            forward(w, 1, k)

    def stage_l(k):
        for w in range(3):
            arrived("g", w, 1, k, 3)
            open_gather(w, 0, k)

    def stage_q(k):
        for w in range(3):
            rest_gather(w, 0, k)
            to_partner(w, k, 0)

    def stage_m(k):
        for w in range(3):
            forward(w, 0, k)

    def stage_n(k):
        for w in range(3):
            arrived("g", w, 0, k, 2)
            for by in (-1, 1):
                to_partner(w, k, by)
        for w in range(3):
            arrived("g", w, 0, k, 3)
            to_partner(w, k, 2)

    def stage_w(k):
        if k == 0:
            for one in small:
                one.wait()

        @pl.loop(0, 5)
        def _(i):
            for w in range(2):
                for side in range(2):
                    block = w_block[w, k, i, side].astype(F32)
                    for t in range(8):
                        turned[w, k, pl.ds(128 * i + 8 * side + t, 8, 16), :] = block[8 * t : 8 * t + 8]

    stages = {n[6:]: f for n, f in locals().items() if n.startswith("stage_")}
    for i, name in enumerate(" ".join(ORDER).lower().split()):
        recycle(LAG if i < 31 else LAG // 2)
        stages[name[0]](int(name[1]))

    recycle(2)
    for w in range(3):
        arrived("end", w)
    for copy, _ in (one for old in leaving for one in old):
        copy.wait_send()


def write_out(*refs):
    copies, sems = [], refs[-1]
    for src, dst in zip(refs[:9], refs[9:18]):
        for at in [(i, j) for i in range(2) for j in range(4)] if len(src.shape) == 7 else [(ALL,)]:
            copies.append(pltpu.make_async_copy(src.at[at], dst.at[at], sems.at[len(copies)]))
            copies[-1].start()
    for one in copies:
        one.wait()


SWAP = (0, 1, 3, 2, 4)


def wide(a):
    return a.reshape(2, 80, 8, 16, ROW).transpose(SWAP).reshape(WIDE)


def tall(a):
    return a.reshape(2, 256, 8, 5, ROW).transpose(SWAP).reshape(TALL)


def wide_small(a):
    return a.reshape(2, 5, 16, ROW).transpose(1, 2, 0, 3).reshape(SMALL[0])


def tall_small(a):
    return a.reshape(2, 2, 8, 5, ROW).transpose(SWAP).reshape(SMALL[2])


def unwide(a):
    return a.reshape(2, 80, 16, 8, ROW).transpose(SWAP).reshape(2, 640, 2048)


def untall(a):
    return a.reshape(2, 256, 5, 8, ROW).transpose(SWAP).reshape(2, 2048, 640)


def unwide_small(a):
    return a.reshape(5, 16, 2, ROW).transpose(2, 0, 1, 3).reshape(2, 5, 2048)


def untall_small(a):
    return a.reshape(2, 2, 5, 8, ROW).transpose(SWAP).reshape(2, 16, 640)


def solution(mesh):
    def step(*arrays):
        big, small = (wide, wide, tall), (wide_small, wide_small, tall_small)
        operands = [f(a[0]) for f, a in zip(big, arrays)] + [f(a) for f, a in zip(big + small * 2, arrays[3:])]
        results = [(s, BF16) for s in (WIDE, WIDE, TALL)] + [(s, F32) for s in SMALL * 2]
        new = pl.pallas_call(
            kernel,
            name="step",
            out_shape=[pltpu.VMEM(s, t) for s, t in results],
            in_specs=[pl.BlockSpec(memory_space=pltpu.HBM)] * 12,
            out_specs=[pl.BlockSpec(memory_space=pltpu.VMEM)] * 9,
            scratch_shapes=[
                *[pltpu.VMEM(s, BF16) for s in HALF * 2],
                *[pltpu.VMEM((2, 3, 2, *s), BF16) for p in PIECE for s in p],
                *[pltpu.VMEM(s, F32) for s in SMALL * 2],
                pltpu.VMEM((2, 3, 80, ROW), BF16),
                pltpu.VMEM((2, 2, 5, 2, 64, ROW), BF16),
                pltpu.VMEM(SMALL[2], BF16),
                pltpu.VMEM((2, 2, 640, ROW), F32),
                pltpu.VMEM((2, 320, ROW), F32),
                *[pltpu.VMEM((2, n, *BOX), BF16) for n in (8, 8, 2, 8)],
                *[pltpu.SemaphoreType.DMA((n,)) for n in (SENDS, RECVS, LOCALS)],
            ],
            compiler_params=pltpu.CompilerParams(collective_id=0, has_side_effects=True, vmem_limit_bytes=44 << 20),
        )(*operands)
        new = pl.pallas_call(
            write_out,
            name="write_out",
            out_shape=[jax.ShapeDtypeStruct(s, t) for s, t in results],
            in_specs=[pl.BlockSpec(memory_space=pl.ANY)] * 9,
            out_specs=[pl.BlockSpec(memory_space=pltpu.HBM)] * 9,
            scratch_shapes=[pltpu.SemaphoreType.DMA((30,))],
            compiler_params=pltpu.CompilerParams(vmem_limit_bytes=1 << 20),
        )(*new)
        back, small_back = (unwide, unwide, untall), (unwide_small, unwide_small, untall_small)
        return tuple(f(a) for f, a in zip(back + small_back * 2, new))

    all_of, cut = P(None, None, None), P(None, "dp", None)
    return jax.shard_map(
        step,
        mesh=mesh,
        in_specs=(P(("rep", "dp"), None, None, None),) * 3 + (all_of,) * 3 + (cut,) * 6,
        out_specs=(P("rep", None, None),) * 3 + (P("rep", "dp", None),) * 6,
        check_vma=False,
    )
```
